128 devices in a mesh: ctx: 32 (over y, z, core), head: 4 (over x).
Axes of the slice: x: 4, y: 4, z: 4, core: 2. Of those that a mesh axis runs over, the one named last changes fastest.
Arguments:
- queries: bfloat16 [32, 32768, 128], P('head', 'ctx'), may hold values from -0.52734375 to 0.52734375
- key_rows: bfloat16 [32, 32768, 128], P('head', 'ctx'), may hold values from -0.52734375 to 0.52734375
- value_rows: bfloat16 [32, 32768, 128], P('head', 'ctx'), may hold values from -0.52734375 to 0.52734375
- level_weight: float32 [6, 32768], P(None, 'ctx'), may hold values from 0.2 to 2
- out_grad: bfloat16 [32, 32768, 128], P('head', 'ctx'), may hold values from -0.52734375 to 0.52734375
Outputs:
- query_grad: bfloat16 [32, 32768, 128], P('head', 'ctx')
- key_grad: bfloat16 [32, 32768, 128], P('head', 'ctx')
- value_grad: bfloat16 [32, 32768, 128], P('head', 'ctx')
- weight_grad: float32 [6, 32768], P(None, 'ctx')
The draws below stay inside these ranges and needn't reach their ends.
All inputs are finite; a program needn't handle non-finite values.
Results may differ from the reference program's by a relative error of at most 0.0057.
Values sent between devices are 32-bit elements; how exact they have to be, the bound alone decides.
A program may use at most 128 MiB of HBM per device.

```python
import math
import jax
import jax.numpy as jnp
import numpy as np
from jax import lax

H = 32
DH = 128
TOK_DEV = 1024
TOKENS = 32768
LEVELS = 5
N_CTX = 32


def steps_of(key, shape, cuts, low, largest):
    factor_of, own = 1.0, jax.random.fold_in(key, 6)
    for position, parts in cuts:
        heights = jnp.exp(jax.random.uniform(jax.random.fold_in(own, position), (parts,), jnp.float32, low / len(cuts), largest / len(cuts)))
        factor_of = factor_of * jnp.repeat(heights, shape[position] // parts).reshape([-1 if axis == position else 1 for axis in range(len(shape))])
    return factor_of


def gaussian(key, dims, width, limit, shards=(), kind=jnp.bfloat16):
    values = width * jax.random.normal(key, dims, jnp.float32)
    if shards:
        values = values * steps_of(key, dims, shards, -0.22, 0.18)
    return jnp.clip(values, -limit, limit).astype(kind)


def setup_inputs(seed: int = 0) -> dict:
    keys = jax.random.split(jax.random.key(seed), 6)
    queries = gaussian(keys[0], (H, TOKENS, DH), (DH ** -0.5), 0.52734375, ((0, 4), (1, 32)))
    key_rows = gaussian(keys[1], (H, TOKENS, DH), (DH ** -0.5), 0.52734375, ((0, 4), (1, 32)))
    value_rows = gaussian(keys[2], (H, TOKENS, DH), (DH ** -0.5), 0.52734375, ((0, 4), (1, 32)))
    level_weight = jnp.clip(jnp.exp(math.log(2.0) - 2.3025851 * jax.random.uniform(keys[3], (LEVELS + 1, TOKENS), jnp.float32) ** steps_of(keys[3], (LEVELS + 1, TOKENS), ((1, 32),), -0.2, 0.2)), 0.2, 2.0)
    out_grad = gaussian(keys[4], (H, TOKENS, DH), ((2 * DH / TOKENS) ** 0.5), 0.52734375, ((0, 4), (1, 32)))
    return dict(queries=queries, key_rows=key_rows, value_rows=value_rows, level_weight=level_weight, out_grad=out_grad)


highest = lax.Precision.HIGHEST


def as_float(array):
    return array.astype(jnp.float32)


def head_part(operands, weights, flag_rows):
    queries, key_rows, value_rows, out_grad, states = operands
    q_f = as_float(queries)
    k_f = as_float(key_rows)
    v_f = as_float(value_rows)
    g_f = as_float(out_grad)
    steps = jnp.arange(TOK_DEV, dtype=jnp.int32)
    causal = (steps[:, None] >= steps[None, :]).astype(jnp.float32)
    scale = causal[None] * weights[0][:, :, None]
    raw = jnp.einsum('ntd,nsd->nts', q_f, k_f, precision=highest)
    attn = (scale * raw).astype(jnp.bfloat16)
    d_attn = jnp.einsum('ntd,nsd->nts', g_f, v_f, precision=highest)
    local_weight = jnp.sum(causal[None] * raw * d_attn, axis=2)
    d_raw = as_float((scale * d_attn).astype(jnp.bfloat16))
    local_q = jnp.einsum('nts,nsd->ntd', d_raw, k_f, precision=highest)
    local_k = jnp.einsum('nts,ntd->nsd', d_raw, q_f, precision=highest)
    local_v = jnp.einsum('nts,ntd->nsd', as_float(attn), g_f, precision=highest)
    z_all = jnp.einsum('nte,lnde->lntd', g_f, as_float(states), precision=highest)
    query_sum = local_q + jnp.sum(weights[1:][:, :, :, None] * z_all, axis=0)
    level_weights = jnp.sum(z_all * q_f[None], axis=3)
    weighted = as_float((weights[1:][:, :, :, None] * g_f[None]).astype(jnp.bfloat16))
    state_grad = jnp.einsum('ntd,lnte->lnde', q_f, weighted, precision=highest)
    state_grad = state_grad * flag_rows[:, :, None, None]
    weight_rows = jnp.concatenate([local_weight[None], level_weights], axis=0)
    return query_sum, local_k, local_v, weight_rows, state_grad


def reference(queries, key_rows, value_rows, level_weight, out_grad):
    def shaped(array):
        return array.reshape(H, N_CTX, TOK_DEV, DH)

    q_all, k_all, v_all, g_all = shaped(queries), shaped(key_rows), shaped(value_rows), shaped(out_grad)
    weights = level_weight.reshape(LEVELS + 1, N_CTX, TOK_DEV)
    group_state = jnp.einsum('hntd,hnte->hnde', as_float(k_all), as_float(v_all), precision=highest)
    positions = np.arange(N_CTX)
    states = []
    flag_list = []
    siblings = []
    for height in range(LEVELS):
        span = 2 ** height
        sums = group_state.reshape(H, N_CTX // span, span, DH, DH).sum(axis=2)
        parity = jnp.asarray((positions // span) % 2, dtype=jnp.float32)
        sibling = (positions // span) ^ 1
        siblings.append(sibling)
        flag_list.append(parity)
        states.append(sums[:, sibling] * parity[None, :, None, None])
    state_bf = jnp.stack(states, axis=1).astype(jnp.bfloat16)
    flag_rows = jnp.stack(flag_list, axis=0)

    def one_head(operands):
        return head_part(operands, weights, flag_rows)

    query_sum, local_k, local_v, weight_rows, state_grad = lax.map(
        one_head, (q_all, k_all, v_all, g_all, state_bf))
    group_grad = jnp.zeros((H, N_CTX, DH, DH), jnp.float32)
    for height in range(LEVELS):
        span = 2 ** height
        sums = state_grad[:, height].reshape(H, N_CTX // span, span, DH, DH).sum(axis=2)
        clear = 1.0 - flag_list[height]
        group_grad = group_grad + sums[:, siblings[height]] * clear[None, :, None, None]
    grad_bf = as_float(group_grad.astype(jnp.bfloat16))
    key_sum = local_k + jnp.einsum('hnse,hnde->hnsd', as_float(v_all), grad_bf, precision=highest)
    value_sum = local_v + jnp.einsum('hnsd,hnde->hnse', as_float(k_all), grad_bf, precision=highest)
    query_grad = query_sum.astype(jnp.bfloat16).reshape(H, N_CTX * TOK_DEV, DH)
    key_grad = key_sum.astype(jnp.bfloat16).reshape(H, N_CTX * TOK_DEV, DH)
    value_grad = value_sum.astype(jnp.bfloat16).reshape(H, N_CTX * TOK_DEV, DH)
    weight_grad = jnp.sum(weight_rows, axis=0).reshape(LEVELS + 1, N_CTX * TOK_DEV)
    return query_grad, key_grad, value_grad, weight_grad
```

```python
import functools

import jax
import jax.numpy as jnp
from jax import lax
from jax.experimental import pallas as pl
from jax.experimental.pallas import tpu as pltpu
from jax.sharding import PartitionSpec as P

F32, BF16 = jnp.float32, jnp.bfloat16
CHUNK = 256


def mm(a, b, ca, cb):
    return lax.dot_general(a, b, (((ca,), (cb,)), ((), ())), preferred_element_type=F32)


def spread_weights(w_ref, wb_ref):
    rows, length = w_ref.shape
    padded = jnp.concatenate([w_ref[...], w_ref[0 : 8 - rows, :]], axis=0)
    columns = padded.T
    for row in range(rows):
        wb_ref[row] = jnp.broadcast_to(columns[:, row : row + 1], (length, 128))


def first_kernel(q_ref, k_ref, v_ref, g_ref, w_ref, gs_ref, sg_ref, wb_ref):
    @pl.when(pl.program_id(0) == 0)
    def _():
        spread_weights(w_ref, wb_ref)

    gs_ref[0] = mm(k_ref[0], v_ref[0], 0, 0)
    levels = sg_ref.shape[0]
    g_f = g_ref[0].astype(F32)
    q_t = q_ref[0].T
    for level in range(levels):
        weighted = (wb_ref[1 + level] * g_f).astype(BF16)
        sg_ref[level, 0] = mm(q_t, weighted, 1, 0)


def last_kernel(q_ref, k_ref, v_ref, g_ref, w_ref, st_ref, gg_ref, qg_ref, kg_ref, vg_ref, wg_ref, wb_ref, acc_ref):
    head = pl.program_id(0)
    levels = st_ref.shape[0]
    length, dim = q_ref.shape[1:]
    chunks = length // CHUNK

    @pl.when(head == 0)
    def _():
        spread_weights(w_ref, wb_ref)
        acc_ref[...] = jnp.zeros_like(acc_ref)

    row = lax.broadcasted_iota(jnp.int32, (CHUNK, CHUNK), 0)
    col = lax.broadcasted_iota(jnp.int32, (CHUNK, CHUNK), 1)
    lower, upper = row >= col, row <= col
    parts = [pl.ds(c * CHUNK, CHUNK) for c in range(chunks)]
    suffix = [gg_ref[0].astype(F32)]
    for c in range(chunks - 1, 0, -1):
        g_0 = (wb_ref[0, parts[c]] * g_ref[0, parts[c]].astype(F32)).astype(BF16)
        suffix.append(suffix[-1] + mm(q_ref[0, parts[c]], g_0, 0, 0))
    suffix = [s.astype(BF16) for s in suffix[::-1]]
    prefix = jnp.zeros((dim, dim), F32)
    states = jnp.concatenate([st_ref[level, 0] for level in range(levels)], axis=0)
    for c in range(chunks):
        rows = parts[c]
        q, k, v, g = (ref[0, rows] for ref in (q_ref, k_ref, v_ref, g_ref))
        w_0 = wb_ref[0, rows]
        q_f = q.astype(F32)
        q_0 = (w_0 * q_f).astype(BF16)
        g_0 = (w_0 * g.astype(F32)).astype(BF16)
        raw_t = jnp.where(upper, mm(k, q, 1, 1), 0.0).astype(BF16)
        vg_ref[0, rows] = (mm(raw_t, g_0, 1, 0) + mm(k, suffix[c], 1, 0)).astype(BF16)
        da_t = jnp.where(upper, mm(v, g, 1, 1), 0.0).astype(BF16)
        kg_ref[0, rows] = (mm(da_t, q_0, 1, 0) + mm(v, suffix[c], 1, 1)).astype(BF16)
        da = jnp.where(lower, mm(g, v, 1, 1), 0.0).astype(BF16)
        z = mm(da, k, 1, 0)
        if c:
            z = z + mm(g, prefix.astype(BF16), 1, 1)
        total = w_0 * z
        acc_ref[0, rows] += q_f * z
        for level in range(levels):
            z = mm(g, states[level * dim : (level + 1) * dim], 1, 1)
            total = total + wb_ref[1 + level, rows] * z
            acc_ref[1 + level, rows] += q_f * z
        qg_ref[0, rows] = total.astype(BF16)
        if c < chunks - 1:
            prefix = prefix + mm(k, v, 0, 0)

    @pl.when(head == pl.num_programs(0) - 1)
    def _():
        ones = jnp.ones((8, dim), BF16)
        for level in range(levels + 1):
            term = acc_ref[level]
            high = term.astype(BF16)
            low = (term - high.astype(F32)).astype(BF16)
            sums = mm(ones, high, 1, 1) + mm(ones, low, 1, 1)
            wg_ref[level : level + 1, :] = sums[0:1]


def first_call(q, k, v, g, w, levels):
    heads, length, dim = q.shape
    block = pl.BlockSpec((1, length, dim), lambda h: (h, 0, 0))
    return pl.pallas_call(
        first_kernel,
        grid=(heads,),
        in_specs=[block] * 4 + [pl.BlockSpec(w.shape, lambda h: (0, 0))],
        out_specs=[
            pl.BlockSpec((1, dim, dim), lambda h: (h, 0, 0)),
            pl.BlockSpec((levels, 1, dim, dim), lambda h: (0, h, 0, 0)),
        ],
        out_shape=[
            jax.ShapeDtypeStruct((heads, dim, dim), F32),
            jax.ShapeDtypeStruct((levels, heads, dim, dim), F32),
        ],
        scratch_shapes=[pltpu.VMEM((levels + 1, length, dim), F32)],
        cost_estimate=pl.CostEstimate(flops=2 * 6 * q.size * dim, bytes_accessed=12 << 20, transcendentals=0),
    )(q, k, v, g, w)


def last_call(q, k, v, g, w, states, grad_bf):
    heads, length, dim = q.shape
    levels = states.shape[0]
    block = pl.BlockSpec((1, length, dim), lambda h: (h, 0, 0))
    whole = pl.BlockSpec(w.shape, lambda h: (0, 0))
    return pl.pallas_call(
        last_kernel,
        grid=(heads,),
        in_specs=[block] * 4
        + [
            whole,
            pl.BlockSpec((levels, 1, dim, dim), lambda h: (0, h, 0, 0)),
            pl.BlockSpec((1, dim, dim), lambda h: (h, 0, 0)),
        ],
        out_specs=[block] * 3 + [whole],
        out_shape=[jax.ShapeDtypeStruct(q.shape, BF16)] * 3 + [jax.ShapeDtypeStruct(w.shape, F32)],
        scratch_shapes=[pltpu.VMEM((levels + 1, length, dim), F32)] * 2,
        cost_estimate=pl.CostEstimate(flops=20 * q.size * dim, bytes_accessed=16 << 20, transcendentals=0),
    )(q, k, v, g, w, states, grad_bf)


def partner_2(shard, axis, distance):
    return lax.ppermute(shard, axis, [(i, i ^ 1 << distance) for i in range(lax.axis_size(axis))])


def per_device(queries, key_rows, value_rows, level_weight, out_grad):
    levels = lax.axis_size("ctx").bit_length() - 1
    position = lax.axis_index("ctx")
    bit_flags = [(position // 2**height % 2).astype(F32) for height in range(levels)]
    group_state, state_grad = first_call(queries, key_rows, value_rows, out_grad, level_weight, levels)
    running = group_state
    states = []
    adjoint = None
    for height in range(levels):
        partner = partner_2(running, "ctx", height)
        states.append(bit_flags[height] * partner)
        running = running + partner
        top = levels - 1 - height
        sent = bit_flags[top] * state_grad[top]
        if adjoint is not None:
            sent = sent + adjoint
        received = partner_2(sent, "ctx", top)
        adjoint = received if adjoint is None else adjoint + received
    query_grad, key_grad, value_grad, rows = last_call(
        queries, key_rows, value_rows, out_grad, level_weight,
        jnp.stack(states, axis=0).astype(BF16), adjoint.astype(BF16),
    )
    return query_grad, key_grad, value_grad, lax.psum(rows, "head")


def solution(mesh):
    rows = P("head", "ctx", None)
    return jax.shard_map(
        per_device,
        mesh=mesh,
        in_specs=(rows, rows, rows, P(None, "ctx"), rows),
        out_specs=(rows, rows, rows, P(None, "ctx")),
        check_vma=False,
    )
```

```python
import functools

import jax
import jax.numpy as jnp
from jax import lax
from jax.experimental import pallas as pl
from jax.experimental.pallas import tpu as pltpu
from jax.sharding import PartitionSpec as P

F32, BF16 = jnp.float32, jnp.bfloat16
CHUNK = 256


def mm(a, b, ca, cb):
    return lax.dot_general(a, b, (((ca,), (cb,)), ((), ())), preferred_element_type=F32)


def spread_weights(w_ref, wb_ref):
    rows, length = w_ref.shape
    padded = jnp.concatenate([w_ref[...], w_ref[0 : 8 - rows, :]], axis=0)
    columns = padded.T
    for row in range(rows):
        wb_ref[row] = jnp.broadcast_to(columns[:, row : row + 1], (length, 128))


def first_kernel(q_ref, k_ref, v_ref, g_ref, w_ref, gs_ref, sg_ref, wb_ref):
    @pl.when(pl.program_id(0) == 0)
    def _():
        spread_weights(w_ref, wb_ref)

    gs_ref[0] = mm(k_ref[0], v_ref[0], 0, 0)
    levels = sg_ref.shape[0]
    g_f = g_ref[0].astype(F32)
    q_t = q_ref[0].T
    for level in range(levels):
        weighted = (wb_ref[1 + level] * g_f).astype(BF16)
        sg_ref[level, 0] = mm(q_t, weighted, 1, 0)


def last_kernel(q_ref, k_ref, v_ref, g_ref, w_ref, st_ref, gg_ref, qg_ref, kg_ref, vg_ref, wg_ref, wb_ref, acc_ref):
    head = pl.program_id(0)
    levels = st_ref.shape[0]
    length, dim = q_ref.shape[1:]
    chunks = length // CHUNK

    @pl.when(head == 0)
    def _():
        spread_weights(w_ref, wb_ref)
        acc_ref[...] = jnp.zeros_like(acc_ref)

    row = lax.broadcasted_iota(jnp.int32, (CHUNK, CHUNK), 0)
    col = lax.broadcasted_iota(jnp.int32, (CHUNK, CHUNK), 1)
    lower, upper = row >= col, row <= col
    parts = [pl.ds(c * CHUNK, CHUNK) for c in range(chunks)]
    suffix = [gg_ref[0].astype(F32)]
    for c in range(chunks - 1, 0, -1):
        g_0 = (wb_ref[0, parts[c]] * g_ref[0, parts[c]].astype(F32)).astype(BF16)
        suffix.append(suffix[-1] + mm(q_ref[0, parts[c]], g_0, 0, 0))
    suffix = [s.astype(BF16) for s in suffix[::-1]]
    prefix = jnp.zeros((dim, dim), F32)
    states = jnp.concatenate([st_ref[level, 0] for level in range(levels)], axis=0)
    for c in range(chunks):
        rows = parts[c]
        q, k, v, g = (ref[0, rows] for ref in (q_ref, k_ref, v_ref, g_ref))
        w_0 = wb_ref[0, rows]
        q_f = q.astype(F32)
        q_0 = (w_0 * q_f).astype(BF16)
        g_0 = (w_0 * g.astype(F32)).astype(BF16)
        raw_t = jnp.where(upper, mm(k, q, 1, 1), 0.0).astype(BF16)
        vg_ref[0, rows] = (mm(raw_t, g_0, 1, 0) + mm(k, suffix[c], 1, 0)).astype(BF16)
        da_t = jnp.where(upper, mm(v, g, 1, 1), 0.0).astype(BF16)
        kg_ref[0, rows] = (mm(da_t, q_0, 1, 0) + mm(v, suffix[c], 1, 1)).astype(BF16)
        da = jnp.where(lower, mm(g, v, 1, 1), 0.0).astype(BF16)
        z = mm(da, k, 1, 0)
        if c:
            z = z + mm(g, prefix.astype(BF16), 1, 1)
        total = w_0 * z
        acc_ref[0, rows] += q_f * z
        for level in range(levels):
            z = mm(g, states[level * dim : (level + 1) * dim], 1, 1)
            total = total + wb_ref[1 + level, rows] * z
            acc_ref[1 + level, rows] += q_f * z
        qg_ref[0, rows] = total.astype(BF16)
        if c < chunks - 1:
            prefix = prefix + mm(k, v, 0, 0)

    @pl.when(head == pl.num_programs(0) - 1)
    def _():
        ones = jnp.ones((8, dim), BF16)
        for level in range(levels + 1):
            term = acc_ref[level]
            high = term.astype(BF16)
            low = (term - high.astype(F32)).astype(BF16)
            sums = mm(ones, high, 1, 1) + mm(ones, low, 1, 1)
            wg_ref[level : level + 1, :] = sums[0:1]


def first_call(q, k, v, g, w, levels):
    heads, length, dim = q.shape
    block = pl.BlockSpec((1, length, dim), lambda h: (h, 0, 0))
    return pl.pallas_call(
        first_kernel,
        grid=(heads,),
        in_specs=[block] * 4 + [pl.BlockSpec(w.shape, lambda h: (0, 0))],
        out_specs=[
            pl.BlockSpec((1, dim, dim), lambda h: (h, 0, 0)),
            pl.BlockSpec((levels, 1, dim, dim), lambda h: (0, h, 0, 0)),
        ],
        out_shape=[
            jax.ShapeDtypeStruct((heads, dim, dim), F32),
            jax.ShapeDtypeStruct((levels, heads, dim, dim), F32),
        ],
        scratch_shapes=[pltpu.VMEM((levels + 1, length, dim), F32)],
        cost_estimate=pl.CostEstimate(flops=2 * 6 * q.size * dim, bytes_accessed=12 << 20, transcendentals=0),
    )(q, k, v, g, w)


def last_call(q, k, v, g, w, states, grad_bf):
    heads, length, dim = q.shape
    levels = states.shape[0]
    block = pl.BlockSpec((1, length, dim), lambda h: (h, 0, 0))
    whole = pl.BlockSpec(w.shape, lambda h: (0, 0))
    return pl.pallas_call(
        last_kernel,
        grid=(heads,),
        in_specs=[block] * 4
        + [
            whole,
            pl.BlockSpec((levels, 1, dim, dim), lambda h: (0, h, 0, 0)),
            pl.BlockSpec((1, dim, dim), lambda h: (h, 0, 0)),
        ],
        out_specs=[block] * 3 + [whole],
        out_shape=[jax.ShapeDtypeStruct(q.shape, BF16)] * 3 + [jax.ShapeDtypeStruct(w.shape, F32)],
        scratch_shapes=[pltpu.VMEM((levels + 1, length, dim), F32)] * 2,
        cost_estimate=pl.CostEstimate(flops=20 * q.size * dim, bytes_accessed=16 << 20, transcendentals=0),
    )(q, k, v, g, w, states, grad_bf)


MESH = pl.DeviceIdType.MESH


class Wires:
    def __init__(self, send_sem, recv_sem):
        self.sems = (send_sem, recv_sem)
        self.count = 0

    def send(self, src, dst, device):
        copy = pltpu.make_async_remote_copy(
            src_ref=src, dst_ref=dst, send_sem=self.sems[0].at[self.count],
            recv_sem=self.sems[1].at[self.count], device_id=device, device_id_type=MESH,
        )
        self.count += 1
        copy.start()
        return copy


def greet(devices):
    barrier = pltpu.get_barrier_semaphore()
    for device in devices:
        pl.semaphore_signal(barrier, inc=1, device_id=device, device_id_type=MESH)
    pl.semaphore_wait(barrier, len(devices))


def gather_start(wires, mine, got, low, high, lower, upper):
    first = (wires.send(mine.at[high], got.at[0, high], upper), wires.send(mine.at[low], got.at[1, low], lower))
    second = (wires.send(mine.at[low], got.at[0, low], upper), wires.send(mine.at[high], got.at[1, high], lower))
    return first, second


def gather_relay(wires, first, got, low, high, lower, upper):
    first[0].wait_recv()
    up = wires.send(got.at[0, high], got.at[2, high], upper)
    first[1].wait_recv()
    down = wires.send(got.at[1, low], got.at[2, low], lower)
    return up, down


def reduce_start(wires, message, relay, got, low, high, lower, upper):
    first = (wires.send(message.at[2, low], relay.at[0], upper), wires.send(message.at[2, high], relay.at[1], lower))
    second = (wires.send(message.at[0, high], got.at[0, high], upper), wires.send(message.at[1, low], got.at[1, low], lower))
    return first, second


def reduce_relay(wires, first, message, relay, got, low, high, lower, upper):
    first[0].wait_recv()
    message[0, low] = message[0, low] + relay[0]
    up = wires.send(message.at[0, low], got.at[0, low], upper)
    first[1].wait_recv()
    message[1, high] = message[1, high] + relay[1]
    down = wires.send(message.at[1, high], got.at[1, high], lower)
    return up, down


def exchange_kernel(gs_ref, sg_ref, st_out, gg_out, gs_in, sg_in, sg0_in, mine_z, mine_y, got_z, got_y,
                    msg_y, msg_z, rel_y, rel_z, back_y, back_z, st, gg, send_sem, recv_sem):
    wires = Wires(send_sem, recv_sem)
    me = lax.axis_index("ctx")
    core, z, y = me % 2, me // 2 % 4, me // 8
    heads = gs_ref.shape[0]
    half = heads // 2
    own, other = pl.ds(half * core, half), pl.ds(half * (1 - core), half)
    low, high = pl.ds(0, half // 2), pl.ds(half // 2, half // 2)

    def at(y, z, core):
        return {"ctx": ((y + 4) % 4 * 4 + (z + 4) % 4) * 2 + core}

    def flag(condition):
        return jnp.where(condition, 1.0, 0.0).astype(F32)

    mate = at(y, z, 1 - core)
    z_ends = (at(y, z - 1, core), at(y, z + 1, core))
    y_ends = (at(y - 1, z, core), at(y + 1, z, core))
    greet((mate, *z_ends, *y_ends))

    d_34 = wires.send(sg_ref.at[pl.ds(3, 2), other], sg_in.at[pl.ds(2, 2)], mate)
    d_gs = wires.send(gs_ref, gs_in, mate)
    d_12 = wires.send(sg_ref.at[pl.ds(1, 2), other], sg_in.at[pl.ds(0, 2)], mate)
    d_0 = wires.send(sg_ref.at[0], sg0_in, mate)

    d_34.wait_recv()
    sum_3 = sg_ref[3, own] + sg_in[2]
    sum_4 = sg_ref[4, own] + sg_in[3]
    msg_y[0] = flag(y == 3) * sum_4
    msg_y[1] = flag(y % 2 == 1) * sum_3 + flag(y == 2) * sum_4
    msg_y[2] = flag(y >= 2) * sum_4
    b_1, b_2 = reduce_start(wires, msg_y, rel_y, back_y, low, high, *y_ends)

    d_gs.wait_recv()
    mine_z[...] = gs_ref[own] + gs_in[own]
    f_1, f_2 = gather_start(wires, mine_z, got_z, low, high, *z_ends)
    b_3 = reduce_relay(wires, b_1, msg_y, rel_y, back_y, low, high, *y_ends)
    f_3 = gather_relay(wires, f_1, got_z, low, high, *z_ends)
    st_out[0] = (flag(core == 1) * gs_in[...]).astype(BF16)
    d_12.wait_recv()

    for copy in (*b_2, *b_3):
        copy.wait_recv()
    adjoint = back_y[0] + back_y[1]
    sum_1 = sg_ref[1, own] + sg_in[0]
    sum_2 = sg_ref[2, own] + sg_in[1]
    msg_z[0] = adjoint + flag(z == 3) * sum_2
    msg_z[1] = adjoint + flag(z % 2 == 1) * sum_1 + flag(z == 2) * sum_2
    msg_z[2] = adjoint + flag(z >= 2) * sum_2
    c_1, c_2 = reduce_start(wires, msg_z, rel_z, back_z, low, high, *z_ends)

    for copy in (*f_2, *f_3):
        copy.wait_recv()
    mine_y[...] = mine_z[...] + got_z[0] + got_z[1] + got_z[2]
    g_1, g_2 = gather_start(wires, mine_y, got_y, low, high, *y_ends)
    st[0, own] = flag(z % 2 == 1) * got_z[0]
    st[1, own] = flag(z >= 2) * got_z[2] + flag(z == 2) * got_z[0] + flag(z == 3) * got_z[1]
    t_1 = wires.send(st.at[pl.ds(0, 2), own], st.at[pl.ds(0, 2), own], mate)
    c_3 = reduce_relay(wires, c_1, msg_z, rel_z, back_z, low, high, *z_ends)
    g_3 = gather_relay(wires, g_1, got_y, low, high, *y_ends)

    for copy in (*c_2, *c_3):
        copy.wait_recv()
    gg[own] = adjoint + back_z[0] + back_z[1]
    t_2 = wires.send(gg.at[own], gg.at[own], mate)
    for copy in (*g_2, *g_3):
        copy.wait_recv()
    st[2, own] = flag(y % 2 == 1) * got_y[0]
    st[3, own] = flag(y >= 2) * got_y[2] + flag(y == 2) * got_y[0] + flag(y == 3) * got_y[1]
    t_3 = wires.send(st.at[pl.ds(2, 2), own], st.at[pl.ds(2, 2), own], mate)
    d_0.wait_recv()
    t_2.wait_recv()
    gg_out[...] = (gg[...] + flag(core == 0) * sg0_in[...]).astype(BF16)
    t_1.wait_recv()
    st_out[1:3] = st[0:2].astype(BF16)
    t_3.wait_recv()
    st_out[3:5] = st[2:4].astype(BF16)
    for copy in (d_34, d_gs, d_12, d_0, *b_1, *b_2, *b_3, *f_1, *f_2, *f_3, *c_1, *c_2, *c_3, *g_1, *g_2, *g_3, t_1, t_2, t_3):
        copy.wait_send()


def exchange_call(group_state, state_grad):
    levels, heads, dim, _ = state_grad.shape
    half = heads // 2
    vmem = pl.BlockSpec(memory_space=pltpu.VMEM)

    def block(*lead):
        return pltpu.VMEM((*lead, dim, dim), F32)

    return pl.pallas_call(
        exchange_kernel,
        in_specs=[vmem] * 2,
        out_specs=[vmem] * 2,
        out_shape=[jax.ShapeDtypeStruct(state_grad.shape, BF16), jax.ShapeDtypeStruct(group_state.shape, BF16)],
        scratch_shapes=[
            block(heads), block(levels - 1, half), block(heads), block(half), block(half), block(3, half), block(3, half),
            block(3, half), block(3, half), block(2, half // 2), block(2, half // 2), block(2, half), block(2, half),
            block(levels - 1, heads), block(heads), pltpu.SemaphoreType.DMA((31,)), pltpu.SemaphoreType.DMA((31,)),
        ],
        compiler_params=pltpu.CompilerParams(collective_id=0, has_side_effects=True),
    )(group_state, state_grad)


def total_kernel(count, rows_ref, out_ref, slots, send_sem, recv_sem):
    wires = Wires(send_sem, recv_sem)
    me = lax.axis_index("head")
    peers = [{"head": (me + step) % count} for step in range(1, count)]
    greet(peers)
    copies = [wires.send(rows_ref, slots.at[me], peer) for peer in peers]
    slots[me] = rows_ref[...]
    for copy in copies:
        copy.wait_recv()
    total = slots[0]
    for index in range(1, count):
        total = total + slots[index]
    out_ref[...] = total
    for copy in copies:
        copy.wait_send()


def total_call(rows, count):
    vmem = pl.BlockSpec(memory_space=pltpu.VMEM)
    return pl.pallas_call(
        functools.partial(total_kernel, count),
        in_specs=[vmem],
        out_specs=vmem,
        out_shape=jax.ShapeDtypeStruct(rows.shape, F32),
        scratch_shapes=[pltpu.VMEM((count, *rows.shape), F32)] + [pltpu.SemaphoreType.DMA((count - 1,))] * 2,
        compiler_params=pltpu.CompilerParams(collective_id=1, has_side_effects=True),
    )(rows)


def per_device(queries, key_rows, value_rows, level_weight, out_grad):
    levels = lax.axis_size("ctx").bit_length() - 1
    group_state, state_grad = first_call(queries, key_rows, value_rows, out_grad, level_weight, levels)
    states, grad_bf = exchange_call(group_state, state_grad)
    query_grad, key_grad, value_grad, rows = last_call(
        queries, key_rows, value_rows, out_grad, level_weight, states, grad_bf)
    return query_grad, key_grad, value_grad, total_call(rows, lax.axis_size("head"))


def solution(mesh):
    rows = P("head", "ctx", None)
    return jax.shard_map(
        per_device,
        mesh=mesh,
        in_specs=(rows, rows, rows, P(None, "ctx"), rows),
        out_specs=(rows, rows, rows, P(None, "ctx")),
        check_vma=False,
    )
```

```python
import jax
import jax.numpy as jnp
from jax import lax
from jax.experimental import pallas as pl
from jax.experimental.pallas import tpu as pltpu
from jax.sharding import PartitionSpec as P

F32, BF16 = jnp.float32, jnp.bfloat16
MESH = pl.DeviceIdType.MESH
CHUNK = 256
ARRIVALS = (
    (0, 0), (0, 1), (0, 2), (1, 0), (0, 3), (1, 1), (1, 2), (2, 0),
    (1, 3), (2, 1), (2, 2), (3, 0), (2, 3), (3, 1), (3, 2), (3, 3),
)


def mm(a, b, ca, cb):
    return lax.dot_general(a, b, (((ca,), (cb,)), ((), ())), preferred_element_type=F32)


def whole_kernel(q_hbm, k_hbm, v_hbm, g_hbm, w_ref, qg_hbm, kg_hbm, vg_hbm, wg_ref,
                 q_ref, k_ref, v_ref, g_ref, qg_ref, kg_ref, vg_ref, tot, pk, pv, wb, acc,
                 loc, in_own, in_other, f_run, f_got, b_msg, b_got, adj, st0, st, gg, prefix, suffix, slots,
                 in_sem, out_sem, d_sem, f_sem, b_sem, s_sem, t_sem, w_sem):
    me, mine = lax.axis_index("ctx"), lax.axis_index("head")
    core, z, y = me % 2, me // 2 % 4, me // 8
    heads, length, dim = q_ref.shape
    half, chunks, levels = heads // 2, length // CHUNK, 5
    parts = [pl.ds(c * CHUNK, CHUNK) for c in range(chunks)]
    own, other = half * core, half * (1 - core)

    def at(y, z, core):
        return {"ctx": (y * 4 + z) * 2 + core}

    def flag(condition):
        return jnp.where(condition, 1.0, 0.0).astype(F32)

    mate = at(y, z, 1 - core)
    z_near, z_far = at(y, z + 1 - 2 * (z % 2), core), at(y, 3 - z, core)
    y_near, y_far = at(y + 1 - 2 * (y % 2), z, core), at(3 - y, z, core)
    f_peer = (z_near, z_far, y_near, y_far)
    b_peer = f_peer[::-1]
    bits = (flag(z % 2 == 1), flag(z >= 2), flag(y % 2 == 1), flag(y >= 2))
    head_count = 4
    head_peers = [{"head": (mine + step) % head_count} for step in range(1, head_count)]

    def remote(src, dst, sems, index, device):
        return pltpu.make_async_remote_copy(
            src_ref=src, dst_ref=dst, send_sem=sems.at[(0, *index)], recv_sem=sems.at[(1, *index)],
            device_id=device, device_id_type=MESH)

    def inputs(h):
        pairs = ((q_hbm, q_ref), (k_hbm, k_ref), (v_hbm, v_ref), (g_hbm, g_ref))
        return [pltpu.make_async_copy(src.at[h], dst.at[h], in_sem.at[h, i]) for i, (src, dst) in enumerate(pairs)]

    def outputs(h, which):
        pairs = ((qg_ref, qg_hbm), (kg_ref, kg_hbm), (vg_ref, vg_hbm))
        return [pltpu.make_async_copy(pairs[i][0].at[h], pairs[i][1].at[h], out_sem.at[h, i]) for i in which]

    def first_half(i):
        return remote(loc.at[other + i], in_own.at[i], d_sem, (i,), mate)

    def second_half(i):
        return remote(loc.at[own + i, pl.ds(0, 2)], in_other.at[i], d_sem, (half + i,), mate)

    def f_copy(s, p):
        return remote(f_run.at[s, p], f_got.at[s, p], f_sem, (s, p), f_peer[s])

    def b_copy(s, p):
        return remote(b_msg.at[s, p], b_got.at[s, p], b_sem, (s, p), b_peer[s])

    def state_copy(s, p):
        return remote(st.at[s, own + p], st.at[s, own + p], s_sem, (s, p), mate)

    def grad_copy(p):
        return remote(gg.at[own + p], gg.at[own + p], t_sem, (p,), mate)

    def row_copy(i):
        return remote(slots.at[mine], slots.at[mine], w_sem, (i,), head_peers[i])

    def start_inputs(i, carry):
        for copy in inputs((other + i) % heads):
            copy.start()
        return carry

    lax.fori_loop(0, heads, start_inputs, 0)
    barrier = pltpu.get_barrier_semaphore()
    greeted = [mate, *f_peer, *head_peers]
    for device in greeted:
        pl.semaphore_signal(barrier, inc=1, device_id=device, device_id_type=MESH)
    w_all = jnp.concatenate([w_ref[...], w_ref[0 : 7 - levels, :]], axis=0)
    columns = w_all.T
    for row in range(levels + 1):
        wb[row] = jnp.broadcast_to(columns[:, row : row + 1], (length, dim))
    pl.semaphore_wait(barrier, len(greeted))

    def phase_one(h):
        for copy in inputs(h):
            copy.wait()
        g_f = g_ref[h].astype(F32)
        q_t = q_ref[h].T
        for pair in (1, 3):
            wide = jnp.concatenate([(wb[1 + pair + i] * g_f).astype(BF16) for i in range(2)], axis=1)
            both = mm(q_t, wide, 1, 0)
            loc[h, 1 + pair] = both[:, :dim]
            loc[h, 2 + pair] = both[:, dim:]
        kv = lower = None
        local = []
        for c in range(chunks):
            rows = parts[c]
            g_c = g_ref[h, rows].astype(F32)
            wide = jnp.concatenate([(wb[i, rows] * g_c).astype(BF16) for i in range(2)], axis=1)
            both = mm(q_t[:, c * CHUNK : (c + 1) * CHUNK], wide, 1, 0)
            local.append(both[:, :dim])
            lower = both[:, dim:] if c == 0 else lower + both[:, dim:]
            product = mm(k_ref[h, rows], v_ref[h, rows], 0, 0)
            kv = product if c == 0 else kv + product
            if c < chunks - 1:
                prefix[h, c] = kv.astype(BF16)
        loc[h, 0] = kv
        loc[h, 1] = lower
        total = None
        for c in range(chunks - 1, 0, -1):
            total = local[c] if total is None else total + local[c]
            suffix[h, c - 1] = total

    def level_sum(p, level):
        return loc[own + p, 1 + level] + in_own[p, 1 + level]

    def mate_part(i, carry):
        phase_one(other + i)
        first_half(i).start()
        return carry

    def own_part(i, carry):
        phase_one(own + i)
        second_half(i).start()
        first_half(i).wait_recv()
        b_msg[0, i] = bits[3] * level_sum(i, 4)
        b_copy(0, i).start()
        f_run[0, i] = loc[own + i, 0] + in_own[i, 0]
        f_copy(0, i).start()
        return carry

    lax.fori_loop(0, half, mate_part, 0)
    lax.fori_loop(0, half, own_part, 0)
    odd = flag(core == 1)
    for i in range(half):
        second_half(i).wait_recv()
        st0[own + i] = (odd * in_own[i, 0]).astype(BF16)
        st0[other + i] = (odd * in_other[i, 0]).astype(BF16)

    tri_row = lax.broadcasted_iota(jnp.int32, (CHUNK, CHUNK), 0)
    tri_col = lax.broadcasted_iota(jnp.int32, (CHUNK, CHUNK), 1)
    lower, upper = tri_row >= tri_col, tri_row <= tri_col

    def block(h, first):
        for c in (first, first + 1):
            rows = parts[c]
            q, k, v, g = (ref[h, rows] for ref in (q_ref, k_ref, v_ref, g_ref))
            w_0 = wb[0, rows]
            q_f = q.astype(F32)
            q_0 = (w_0 * q_f).astype(BF16)
            g_0 = (w_0 * g.astype(F32)).astype(BF16)
            raw_t = jnp.where(upper, mm(k, q, 1, 1), 0.0).astype(BF16)
            pv[h, rows] = mm(raw_t, g_0, 1, 0)
            da_t = jnp.where(upper, mm(v, g, 1, 1), 0.0).astype(BF16)
            pk[h, rows] = mm(da_t, q_0, 1, 0)
            da = jnp.where(lower, mm(g, v, 1, 1), 0.0).astype(BF16)
            z_0 = mm(da, k, 1, 0)
            if c:
                both = mm(g, jnp.concatenate([prefix[h, c - 1], st0[h]], axis=0), 1, 1)
                z_0, z_1 = z_0 + both[:, :dim], both[:, dim:]
            else:
                z_1 = mm(g, st0[h], 1, 1)
            tot[h, rows] = w_0 * z_0 + wb[1, rows] * z_1
            if h == 0:
                acc[0, rows] = q_f * z_0
                acc[1, rows] = q_f * z_1
            else:
                acc[0, rows] += q_f * z_0
                acc[1, rows] += q_f * z_1

    def level_pair(h, stage, fresh):
        both_states = jnp.concatenate([st[stage, h], st[stage + 1, h]], axis=0).astype(BF16)
        row = 2 + stage
        for rows in parts:
            both = mm(g_ref[h, rows], both_states, 1, 1)
            q_f = q_ref[h, rows].astype(F32)
            total = tot[h, rows]
            for i in range(2):
                z_i = both[:, i * dim : (i + 1) * dim]
                total = total + wb[row + i, rows] * z_i
                if fresh:
                    acc[row + i, rows] = q_f * z_i
                else:
                    acc[row + i, rows] += q_f * z_i
            if stage == 0:
                tot[h, rows] = total
            else:
                qg_ref[h, rows] = total.astype(BF16)
        if stage:
            for copy in outputs(h, (0,)):
                copy.start()

    def apply(h, grad_0):
        grad = gg[h] + flag(core == 0) * grad_0
        zero = jnp.zeros((dim, dim), BF16)
        for c, rows in enumerate(parts):
            x = (grad + suffix[h, c] if c < chunks - 1 else grad).astype(BF16)
            wide = jnp.concatenate([jnp.concatenate([x.T, zero], axis=1), jnp.concatenate([zero, x], axis=1)], axis=0)
            both = mm(jnp.concatenate([v_ref[h, rows], k_ref[h, rows]], axis=1), wide, 1, 0)
            kg_ref[h, rows] = (pk[h, rows] + both[:, :dim]).astype(BF16)
            vg_ref[h, rows] = (pv[h, rows] + both[:, dim:]).astype(BF16)
        for copy in outputs(h, (1, 2)):
            copy.start()

    def take_up(s, p):
        f_copy(s, p).wait_recv()
        got = f_got[s, p]
        if s < 3:
            f_run[s + 1, p] = f_run[s, p] + got
            f_copy(s + 1, p).start()
        st[s, own + p] = bits[s] * got
        state_copy(s, p).start()
        b_copy(s, p).wait_recv()
        total = b_got[s, p] if s == 0 else adj[p] + b_got[s, p]
        if s < 3:
            adj[p] = total
            b_msg[s + 1, p] = total + bits[2 - s] * level_sum(p, 3 - s)
            b_copy(s + 1, p).start()
        else:
            gg[own + p] = total
            grad_copy(p).start()

    work = [(h, c) for h in range(heads) for c in range(0, chunks, 2)]
    for _ in range(3):
        block(*work.pop(0))
    for s, p in ARRIVALS:
        take_up(s, p)
        if work:
            block(*work.pop(0))
        if s == 3:
            for stage in (0, 1):
                state_copy(stage, p).wait_recv()
            level_pair(own + p, 0, p == 0)
            level_pair(other + p, 0, False)
    while work:
        block(*work.pop(0))
    for p in range(half):
        level_pair(own + p, 2, p == 0)
    for p in range(half):
        for stage in (2, 3):
            state_copy(stage, p).wait_recv()
        level_pair(other + p, 2, False)
    ones = jnp.ones((8, dim), BF16)
    for row in range(levels + 1):
        term = acc[row]
        high = term.astype(BF16)
        low = (term - high.astype(F32)).astype(BF16)
        sums = mm(ones, high, 1, 1) + mm(ones, low, 1, 1)
        slots[mine, row : row + 1, :] = sums[0:1]
    for i in range(head_count - 1):
        row_copy(i).start()
    for p in range(half):
        apply(own + p, in_own[p, 1])
    for p in range(half):
        grad_copy(p).wait_recv()
        apply(other + p, in_other[p, 1])
    for i in range(head_count - 1):
        row_copy(i).wait_recv()
    total = slots[0]
    for index in range(1, head_count):
        total = total + slots[index]
    wg_ref[...] = total

    for i in range(half):
        first_half(i).wait_send()
        second_half(i).wait_send()
        grad_copy(i).wait_send()
    for s, p in ARRIVALS:
        f_copy(s, p).wait_send()
        b_copy(s, p).wait_send()
        state_copy(s, p).wait_send()
    for i in range(head_count - 1):
        row_copy(i).wait_send()
    for h in range(heads):
        for copy in outputs(h, (0, 1, 2)):
            copy.wait()


def per_device(queries, key_rows, value_rows, level_weight, out_grad):
    heads, length, dim = queries.shape
    half, rows = heads // 2, level_weight.shape[0]
    vmem, hbm = pl.BlockSpec(memory_space=pltpu.VMEM), pl.BlockSpec(memory_space=pl.ANY)

    def f32(*shape):
        return pltpu.VMEM(shape, F32)

    def square(*lead):
        return f32(*lead, dim, dim)

    def pairs(*shape):
        return pltpu.SemaphoreType.DMA((2, *shape))

    tokens = pltpu.VMEM((heads, length, dim), BF16)
    query_grad, key_grad, value_grad, weight_grad = pl.pallas_call(
        whole_kernel,
        in_specs=[hbm] * 4 + [vmem],
        out_specs=[hbm] * 3 + [vmem],
        out_shape=[jax.ShapeDtypeStruct(queries.shape, BF16)] * 3 + [jax.ShapeDtypeStruct(level_weight.shape, F32)],
        scratch_shapes=[tokens] * 7
        + [f32(heads, length, dim)] * 3
        + [f32(rows, length, dim)] * 2
        + [square(heads, 6), square(half, 6), square(half, 2)]
        + [square(4, half)] * 4
        + [square(half), pltpu.VMEM((heads, dim, dim), BF16), square(4, heads), square(heads)]
        + [pltpu.VMEM((heads, length // CHUNK - 1, dim, dim), BF16), square(heads, length // CHUNK - 1)]
        + [f32(4, rows, length)]
        + [pltpu.SemaphoreType.DMA((heads, 4)), pltpu.SemaphoreType.DMA((heads, 3))]
        + [pairs(heads), pairs(4, half), pairs(4, half), pairs(4, half), pairs(half), pairs(3)],
        compiler_params=pltpu.CompilerParams(
            collective_id=0, has_side_effects=True, vmem_limit_bytes=62 << 20),
    )(queries, key_rows, value_rows, out_grad, level_weight)
    return query_grad, key_grad, value_grad, weight_grad


def solution(mesh):
    rows = P("head", "ctx", None)
    return jax.shard_map(
        per_device,
        mesh=mesh,
        in_specs=(rows, rows, rows, P(None, "ctx"), rows),
        out_specs=(rows, rows, rows, P(None, "ctx")),
        check_vma=False,
    )
```

```python
import jax
import jax.numpy as jnp
from jax import lax
from jax.experimental import pallas as pl
from jax.experimental.pallas import tpu as pltpu
from jax.sharding import PartitionSpec as P

F32, BF16 = jnp.float32, jnp.bfloat16
MESH = pl.DeviceIdType.MESH
CHUNK = 256
ARRIVALS = (
    (0, 0), (0, 1), (0, 2), (1, 0), (0, 3), (1, 1), (1, 2), (2, 0),
    (1, 3), (2, 1), (2, 2), (3, 0), (2, 3), (3, 1), (3, 2), (3, 3),
)

BLOCKS = (2, 1, 1, 1, 1, 1, 1, 1, 1, 1, 1, 0, 3, 0, 0, 0)
MIDDLES = ((),) * 11 + ((0,), (), (1, 2), (3,), ())


def mm(a, b, ca, cb):
    return lax.dot_general(a, b, (((ca,), (cb,)), ((), ())), preferred_element_type=F32)


def whole_kernel(q_hbm, k_hbm, v_hbm, g_hbm, w_ref, qg_ref, kg_ref, vg_ref, wg_ref,
                 q_ref, k_ref, v_ref, g_ref, tot, pk, pv, wb, acc,
                 loc, in_own, in_other, f_run, f_got, b_msg, b_got, adj, st0, st, gg, prefix, suffix, slots,
                 in_sem, d_sem, f_sem, b_sem, s_sem, t_sem, w_sem):
    me, mine = lax.axis_index("ctx"), lax.axis_index("head")
    core, z, y = me % 2, me // 2 % 4, me // 8
    heads, length, dim = q_ref.shape
    half, chunks, levels = heads // 2, length // CHUNK, 5
    parts = [pl.ds(c * CHUNK, CHUNK) for c in range(chunks)]
    own, other = half * core, half * (1 - core)

    def at(y, z, core):
        return {"ctx": (y * 4 + z) * 2 + core}

    def flag(condition):
        return jnp.where(condition, 1.0, 0.0).astype(F32)

    mate = at(y, z, 1 - core)
    z_near, z_far = at(y, z + 1 - 2 * (z % 2), core), at(y, 3 - z, core)
    y_near, y_far = at(y + 1 - 2 * (y % 2), z, core), at(3 - y, z, core)
    f_peer = (z_near, z_far, y_near, y_far)
    b_peer = f_peer[::-1]
    bits = (flag(z % 2 == 1), flag(z >= 2), flag(y % 2 == 1), flag(y >= 2))
    head_count = 4
    head_peers = [{"head": (mine + step) % head_count} for step in range(1, head_count)]

    def remote(src, dst, sems, index, device):
        return pltpu.make_async_remote_copy(
            src_ref=src, dst_ref=dst, send_sem=sems.at[(0, *index)], recv_sem=sems.at[(1, *index)],
            device_id=device, device_id_type=MESH)

    def inputs(h):
        pairs = ((q_hbm, q_ref), (k_hbm, k_ref), (v_hbm, v_ref), (g_hbm, g_ref))
        return [pltpu.make_async_copy(src.at[h], dst.at[h], in_sem.at[h, i]) for i, (src, dst) in enumerate(pairs)]

    def early_copy(i):
        return remote(loc.at[other + i, pl.ds(0, 3)], in_own.at[i, pl.ds(0, 3)], d_sem, (i,), mate)

    def late_copy(i):
        return remote(loc.at[other + i, pl.ds(3, 3)], in_own.at[i, pl.ds(3, 3)], d_sem, (half + i,), mate)

    def low_copy(i):
        return remote(loc.at[own + i, pl.ds(2, 2)], in_other.at[i], d_sem, (2 * half + i,), mate)

    def f_copy(s, p):
        return remote(f_run.at[s, p], f_got.at[s, p], f_sem, (s, p), f_peer[s])

    def b_copy(s, p):
        return remote(b_msg.at[s, p], b_got.at[s, p], b_sem, (s, p), b_peer[s])

    def state_copy(s, p):
        return remote(st.at[s, own + p], st.at[s, own + p], s_sem, (s, p), mate)

    def grad_copy(p):
        return remote(gg.at[own + p], gg.at[own + p], t_sem, (p,), mate)

    def row_copy(i):
        return remote(slots.at[mine], slots.at[mine], w_sem, (i,), head_peers[i])

    def start_inputs(i, carry):
        for copy in inputs((other + i) % heads):
            copy.start()
        return carry

    lax.fori_loop(0, heads, start_inputs, 0)
    barrier = pltpu.get_barrier_semaphore()
    greeted = [mate, *f_peer, *head_peers]
    for device in greeted:
        pl.semaphore_signal(barrier, inc=1, device_id=device, device_id_type=MESH)
    w_all = jnp.concatenate([w_ref[...], w_ref[0 : 7 - levels, :]], axis=0)
    columns = w_all.T
    for row in range(levels + 1):
        wb[row] = jnp.broadcast_to(columns[:, row : row + 1], (length, dim))

    def weighted_pair(h, rows, levels):
        g_f = g_ref[h, rows].astype(F32)
        return jnp.concatenate([(wb[level, rows] * g_f).astype(BF16) for level in levels], axis=1)

    def upper_levels(h):
        for copy in inputs(h):
            copy.wait()
        both = mm(q_ref[h].T, weighted_pair(h, pl.ds(0, length), (4, 5)), 1, 0)
        loc[h, 0] = both[:, :dim]
        loc[h, 1] = both[:, dim:]
        kv = None
        for c, rows in enumerate(parts):
            product = mm(k_ref[h, rows], v_ref[h, rows], 0, 0)
            kv = product if c == 0 else kv + product
            if c < chunks - 1:
                prefix[h, c] = kv.astype(BF16)
        loc[h, 2] = kv

    def lower_levels(h):
        q_t = q_ref[h].T
        both = mm(q_t, weighted_pair(h, pl.ds(0, length), (2, 3)), 1, 0)
        loc[h, 4] = both[:, :dim]
        loc[h, 5] = both[:, dim:]
        level_0 = total = None
        for c in range(chunks - 1, -1, -1):
            both = mm(q_t[:, c * CHUNK : (c + 1) * CHUNK], weighted_pair(h, parts[c], (0, 1)), 1, 0)
            level_0 = both[:, dim:] if level_0 is None else level_0 + both[:, dim:]
            if c:
                total = both[:, :dim] if total is None else total + both[:, :dim]
                suffix[h, c - 1] = total
        loc[h, 3] = level_0

    def level_sum(p, level):
        index = (3, 4, 5, 0, 1)[level]
        return loc[own + p, index] + in_own[p, index]

    def mate_early(i, carry):
        upper_levels(other + i)
        return carry

    def mate_early_send(i, carry):
        upper_levels(other + i)
        early_copy(i).start()
        return carry

    def own_early(i, carry):
        upper_levels(own + i)
        early_copy(i).wait_recv()
        b_msg[0, i] = bits[3] * level_sum(i, 4)
        b_copy(0, i).start()
        f_run[0, i] = loc[own + i, 2] + in_own[i, 2]
        f_copy(0, i).start()
        return carry

    def mate_late(i, carry):
        lower_levels(other + i)
        late_copy(i).start()
        return carry

    def own_late(i, carry):
        lower_levels(own + i)
        low_copy(i).start()
        return carry

    lax.fori_loop(0, 2, mate_early, 0)
    pl.semaphore_wait(barrier, len(greeted))
    for i in range(2):
        early_copy(i).start()
    lax.fori_loop(2, half, mate_early_send, 0)
    lax.fori_loop(0, half, own_early, 0)
    lax.fori_loop(0, half, mate_late, 0)
    lax.fori_loop(0, half, own_late, 0)
    odd = flag(core == 1)
    for i in range(half):
        st0[own + i] = (odd * in_own[i, 2]).astype(BF16)
        low_copy(i).wait_recv()
        st0[other + i] = (odd * in_other[i, 0]).astype(BF16)
        late_copy(i).wait_recv()

    tri_row = lax.broadcasted_iota(jnp.int32, (CHUNK, CHUNK), 0)
    tri_col = lax.broadcasted_iota(jnp.int32, (CHUNK, CHUNK), 1)
    lower, upper = tri_row >= tri_col, tri_row <= tri_col

    def block(h, first):
        for c in (first, first + 1):
            rows = parts[c]
            q, k, v, g = (ref[h, rows] for ref in (q_ref, k_ref, v_ref, g_ref))
            w_0 = wb[0, rows]
            q_f = q.astype(F32)
            q_0 = (w_0 * q_f).astype(BF16)
            g_0 = (w_0 * g.astype(F32)).astype(BF16)
            raw_t = jnp.where(upper, mm(k, q, 1, 1), 0.0).astype(BF16)
            pv[h, rows] = mm(raw_t, g_0, 1, 0)
            da_t = jnp.where(upper, mm(v, g, 1, 1), 0.0).astype(BF16)
            pk[h, rows] = mm(da_t, q_0, 1, 0)
            da = jnp.where(lower, mm(g, v, 1, 1), 0.0).astype(BF16)
            z_0 = mm(da, k, 1, 0)
            if c:
                both = mm(g, jnp.concatenate([prefix[h, c - 1], st0[h]], axis=0), 1, 1)
                z_0, z_1 = z_0 + both[:, :dim], both[:, dim:]
            else:
                z_1 = mm(g, st0[h], 1, 1)
            tot[h, rows] = w_0 * z_0 + wb[1, rows] * z_1
            if h == 0:
                acc[0, rows] = q_f * z_0
                acc[1, rows] = q_f * z_1
            else:
                acc[0, rows] += q_f * z_0
                acc[1, rows] += q_f * z_1

    def level_pair(h, stage, fresh):
        both_states = jnp.concatenate([st[stage, h], st[stage + 1, h]], axis=0).astype(BF16)
        row = 2 + stage
        for rows in parts:
            both = mm(g_ref[h, rows], both_states, 1, 1)
            q_f = q_ref[h, rows].astype(F32)
            total = tot[h, rows]
            for i in range(2):
                z_i = both[:, i * dim : (i + 1) * dim]
                total = total + wb[row + i, rows] * z_i
                if fresh:
                    acc[row + i, rows] = q_f * z_i
                else:
                    acc[row + i, rows] += q_f * z_i
            if stage == 0:
                tot[h, rows] = total
            else:
                qg_ref[h, rows] = total.astype(BF16)

    def apply(h, grad_0):
        grad = gg[h] + flag(core == 0) * grad_0
        zero = jnp.zeros((dim, dim), BF16)
        for c, rows in enumerate(parts):
            x = (grad + suffix[h, c] if c < chunks - 1 else grad).astype(BF16)
            wide = jnp.concatenate([jnp.concatenate([x.T, zero], axis=1), jnp.concatenate([zero, x], axis=1)], axis=0)
            both = mm(jnp.concatenate([v_ref[h, rows], k_ref[h, rows]], axis=1), wide, 1, 0)
            kg_ref[h, rows] = (pk[h, rows] + both[:, :dim]).astype(BF16)
            vg_ref[h, rows] = (pv[h, rows] + both[:, dim:]).astype(BF16)

    def take_up(s, p):
        f_copy(s, p).wait_recv()
        got = f_got[s, p]
        if s < 3:
            f_run[s + 1, p] = f_run[s, p] + got
            f_copy(s + 1, p).start()
        st[s, own + p] = bits[s] * got
        state_copy(s, p).start()
        b_copy(s, p).wait_recv()
        total = b_got[s, p] if s == 0 else adj[p] + b_got[s, p]
        if s < 3:
            adj[p] = total
            b_msg[s + 1, p] = total + bits[2 - s] * level_sum(p, 3 - s)
            b_copy(s + 1, p).start()
        else:
            gg[own + p] = total
            grad_copy(p).start()

    def middle(p):
        for stage in (0, 1):
            state_copy(stage, p).wait_recv()
        level_pair(own + p, 0, p == 0)
        level_pair(other + p, 0, False)

    work = [(h, c) for h in range(heads) for c in range(0, chunks, 2)]
    block(*work.pop(0))
    for index, (s, p) in enumerate(ARRIVALS):
        take_up(s, p)
        for _ in range(BLOCKS[index]):
            block(*work.pop(0))
        for piece in MIDDLES[index]:
            middle(piece)
    for p in range(half):
        level_pair(own + p, 2, p == 0)
    for p in range(half):
        for stage in (2, 3):
            state_copy(stage, p).wait_recv()
        level_pair(other + p, 2, False)
    ones = jnp.ones((8, dim), BF16)
    for row in range(levels + 1):
        term = acc[row]
        high = term.astype(BF16)
        low = (term - high.astype(F32)).astype(BF16)
        sums = mm(ones, high, 1, 1) + mm(ones, low, 1, 1)
        slots[mine, row : row + 1, :] = sums[0:1]
    for i in range(head_count - 1):
        row_copy(i).start()
    for p in range(half):
        apply(own + p, in_own[p, 3])
    for p in range(half):
        grad_copy(p).wait_recv()
        apply(other + p, in_other[p, 1])
    for i in range(head_count - 1):
        row_copy(i).wait_recv()
    total = slots[0]
    for index in range(1, head_count):
        total = total + slots[index]
    wg_ref[...] = total

    for i in range(half):
        early_copy(i).wait_send()
        late_copy(i).wait_send()
        low_copy(i).wait_send()
        grad_copy(i).wait_send()
    for s, p in ARRIVALS:
        f_copy(s, p).wait_send()
        b_copy(s, p).wait_send()
        state_copy(s, p).wait_send()
    for i in range(head_count - 1):
        row_copy(i).wait_send()


def copy_out_kernel(*refs):
    count = len(refs) // 2
    sems = refs[-1]
    copies = [pltpu.make_async_copy(refs[i], refs[count + i], sems.at[i]) for i in range(count)]
    for copy in copies:
        copy.start()
    for copy in copies:
        copy.wait()


def copy_out(arrays):
    return pl.pallas_call(
        copy_out_kernel,
        in_specs=[pl.BlockSpec(memory_space=pltpu.VMEM)] * len(arrays),
        out_specs=[pl.BlockSpec(memory_space=pl.ANY)] * len(arrays),
        out_shape=[jax.ShapeDtypeStruct(array.shape, array.dtype) for array in arrays],
        scratch_shapes=[pltpu.SemaphoreType.DMA((len(arrays),))],
        compiler_params=pltpu.CompilerParams(vmem_limit_bytes=1 << 20),
    )(*arrays)


def per_device(queries, key_rows, value_rows, level_weight, out_grad):
    heads, length, dim = queries.shape
    half, rows = heads // 2, level_weight.shape[0]
    vmem, hbm = pl.BlockSpec(memory_space=pltpu.VMEM), pl.BlockSpec(memory_space=pltpu.HBM)

    def f32(*shape):
        return pltpu.VMEM(shape, F32)

    def square(*lead):
        return f32(*lead, dim, dim)

    def pairs(*shape):
        return pltpu.SemaphoreType.DMA((2, *shape))

    tokens = pltpu.VMEM((heads, length, dim), BF16)
    arrays = pl.pallas_call(
        whole_kernel,
        in_specs=[hbm] * 4 + [vmem],
        out_specs=[vmem] * 4,
        out_shape=[jax.ShapeDtypeStruct(queries.shape, BF16)] * 3 + [jax.ShapeDtypeStruct(level_weight.shape, F32)],
        scratch_shapes=[tokens] * 4
        + [f32(heads, length, dim)] * 3
        + [f32(rows, length, dim)] * 2
        + [square(heads, 6), square(half, 6), square(half, 2)]
        + [square(4, half)] * 4
        + [square(half), pltpu.VMEM((heads, dim, dim), BF16), square(4, heads), square(heads)]
        + [pltpu.VMEM((heads, length // CHUNK - 1, dim, dim), BF16), square(heads, length // CHUNK - 1)]
        + [f32(4, rows, length)]
        + [pltpu.SemaphoreType.DMA((heads, 4))]
        + [pairs(3 * half), pairs(4, half), pairs(4, half), pairs(4, half), pairs(half), pairs(3)],
        compiler_params=pltpu.CompilerParams(
            collective_id=0, has_side_effects=True, vmem_limit_bytes=44 << 20),
    )(queries, key_rows, value_rows, out_grad, level_weight)
    return tuple(copy_out(arrays))


def solution(mesh):
    rows = P("head", "ctx", None)
    return jax.shard_map(
        per_device,
        mesh=mesh,
        in_specs=(rows, rows, rows, P(None, "ctx"), rows),
        out_specs=(rows, rows, rows, P(None, "ctx")),
        check_vma=False,
    )
```

```python
import jax
import jax.numpy as jnp
from jax import lax
from jax.experimental import pallas as pl
from jax.experimental.pallas import tpu as pltpu
from jax.sharding import PartitionSpec as P

F32, BF16 = jnp.float32, jnp.bfloat16
MESH = pl.DeviceIdType.MESH
CHUNK = 256
ARRIVALS = (
    (0, 0), (0, 1), (0, 2), (1, 0), (0, 3), (1, 1), (1, 2), (2, 0),
    (1, 3), (2, 1), (2, 2), (3, 0), (2, 3), (3, 1), (3, 2), (3, 3),
)

BLOCKS = (2, 1, 1, 1, 1, 1, 1, 1, 1, 1, 1, 0, 3, 0, 0, 0)
MIDDLES = ((),) * 11 + ((0,), (), (1, 2), (3,), ())


def mm(a, b, ca, cb):
    return lax.dot_general(a, b, (((ca,), (cb,)), ((), ())), preferred_element_type=F32)


def whole_kernel(q_hbm, k_hbm, v_hbm, g_hbm, w_ref, qg_ref, kg_ref, vg_ref, wg_ref,
                 q_ref, k_ref, v_ref, g_ref, tot, pk, pv, wb, acc,
                 loc, in_own, in_other, f_run, f_got, b_msg, b_got, adj, st0, st, gg, prefix, suffix, slots,
                 in_sem, d_sem, f_sem, b_sem, s_sem, t_sem, w_sem):
    me, mine = lax.axis_index("ctx"), lax.axis_index("head")
    core, z, y = me % 2, me // 2 % 4, me // 8
    heads, length, dim = q_ref.shape
    half, chunks, levels = heads // 2, length // CHUNK, 5
    parts = [pl.ds(c * CHUNK, CHUNK) for c in range(chunks)]
    own, other = half * core, half * (1 - core)

    def at(y, z, core):
        return {"ctx": (y * 4 + z) * 2 + core}

    def flag(condition):
        return jnp.where(condition, 1.0, 0.0).astype(F32)

    mate = at(y, z, 1 - core)
    z_near, z_far = at(y, z + 1 - 2 * (z % 2), core), at(y, 3 - z, core)
    y_near, y_far = at(y + 1 - 2 * (y % 2), z, core), at(3 - y, z, core)
    f_peer = (z_near, z_far, y_near, y_far)
    b_peer = f_peer[::-1]
    bits = (flag(z % 2 == 1), flag(z >= 2), flag(y % 2 == 1), flag(y >= 2))
    head_count = 4
    head_peers = [{"head": (mine + step) % head_count} for step in range(1, head_count)]

    def remote(src, dst, sems, index, device):
        return pltpu.make_async_remote_copy(
            src_ref=src, dst_ref=dst, send_sem=sems.at[(0, *index)], recv_sem=sems.at[(1, *index)],
            device_id=device, device_id_type=MESH)

    def inputs(h):
        pairs = ((q_hbm, q_ref), (k_hbm, k_ref), (v_hbm, v_ref), (g_hbm, g_ref))
        return [pltpu.make_async_copy(src.at[h], dst.at[h], in_sem.at[h, i]) for i, (src, dst) in enumerate(pairs)]

    def early_copy(i):
        return remote(loc.at[other + i, pl.ds(0, 3)], in_own.at[i, pl.ds(0, 3)], d_sem, (i,), mate)

    def late_copy(i):
        return remote(loc.at[other + i, pl.ds(3, 3)], in_own.at[i, pl.ds(3, 3)], d_sem, (half + i,), mate)

    def low_copy(i):
        return remote(loc.at[own + i, pl.ds(2, 2)], in_other.at[i], d_sem, (2 * half + i,), mate)

    def f_copy(s, p):
        return remote(f_run.at[s, p], f_got.at[s, p], f_sem, (s, p), f_peer[s])

    def b_copy(s, p):
        return remote(b_msg.at[s, p], b_got.at[s, p], b_sem, (s, p), b_peer[s])

    def state_copy(s, p):
        return remote(st.at[s, own + p], st.at[s, own + p], s_sem, (s, p), mate)

    def grad_copy(p):
        return remote(gg.at[own + p], gg.at[own + p], t_sem, (p,), mate)

    def row_copy(i):
        return remote(slots.at[mine], slots.at[mine], w_sem, (i,), head_peers[i])

    def start_inputs(i, carry):
        for copy in inputs((other + i) % heads):
            copy.start()
        return carry

    lax.fori_loop(0, heads, start_inputs, 0)
    barrier = pltpu.get_barrier_semaphore()
    greeted = [mate, *f_peer, *head_peers]
    for device in greeted:
        pl.semaphore_signal(barrier, inc=1, device_id=device, device_id_type=MESH)
    w_all = jnp.concatenate([w_ref[...], w_ref[0 : 7 - levels, :]], axis=0)
    columns = w_all.T
    for row in range(levels + 1):
        wb[row] = jnp.broadcast_to(columns[:, row : row + 1], (length, dim))

    def weighted_pair(h, rows, levels):
        g_f = g_ref[h, rows].astype(F32)
        return jnp.concatenate([(wb[level, rows] * g_f).astype(BF16) for level in levels], axis=1)

    def upper_levels(h):
        for copy in inputs(h):
            copy.wait()
        both = mm(q_ref[h].T, weighted_pair(h, pl.ds(0, length), (4, 5)), 1, 0)
        loc[h, 0] = both[:, :dim]
        loc[h, 1] = both[:, dim:]
        kv = None
        for c, rows in enumerate(parts):
            product = mm(k_ref[h, rows], v_ref[h, rows], 0, 0)
            kv = product if c == 0 else kv + product
            if c < chunks - 1:
                prefix[h, c] = kv.astype(BF16)
        loc[h, 2] = kv

    def lower_levels(h):
        q_t = q_ref[h].T
        both = mm(q_t, weighted_pair(h, pl.ds(0, length), (2, 3)), 1, 0)
        loc[h, 4] = both[:, :dim]
        loc[h, 5] = both[:, dim:]
        level_0 = total = None
        for c in range(chunks - 1, -1, -1):
            both = mm(q_t[:, c * CHUNK : (c + 1) * CHUNK], weighted_pair(h, parts[c], (0, 1)), 1, 0)
            level_0 = both[:, dim:] if level_0 is None else level_0 + both[:, dim:]
            if c:
                total = both[:, :dim] if total is None else total + both[:, :dim]
                suffix[h, c - 1] = total
        loc[h, 3] = level_0

    def level_sum(p, level):
        index = (3, 4, 5, 0, 1)[level]
        return loc[own + p, index] + in_own[p, index]

    def mate_early(i, carry):
        upper_levels(other + i)
        return carry

    def mate_early_send(i, carry):
        upper_levels(other + i)
        early_copy(i).start()
        return carry

    def own_early(i, carry):
        upper_levels(own + i)
        early_copy(i).wait_recv()
        b_msg[0, i] = bits[3] * level_sum(i, 4)
        b_copy(0, i).start()
        f_run[0, i] = loc[own + i, 2] + in_own[i, 2]
        f_copy(0, i).start()
        return carry

    def mate_late(i, carry):
        lower_levels(other + i)
        late_copy(i).start()
        return carry

    def own_late(i, carry):
        lower_levels(own + i)
        low_copy(i).start()
        return carry

    lax.fori_loop(0, 2, mate_early, 0)
    pl.semaphore_wait(barrier, len(greeted))
    for i in range(2):
        early_copy(i).start()
    lax.fori_loop(2, half, mate_early_send, 0)
    lax.fori_loop(0, half, own_early, 0)
    lax.fori_loop(0, half, mate_late, 0)
    lax.fori_loop(0, half, own_late, 0)
    odd = flag(core == 1)
    for i in range(half):
        st0[own + i] = (odd * in_own[i, 2]).astype(BF16)
        low_copy(i).wait_recv()
        st0[other + i] = (odd * in_other[i, 0]).astype(BF16)
        late_copy(i).wait_recv()

    tri_row = lax.broadcasted_iota(jnp.int32, (CHUNK, CHUNK), 0)
    tri_col = lax.broadcasted_iota(jnp.int32, (CHUNK, CHUNK), 1)
    lower, upper = tri_row >= tri_col, tri_row <= tri_col

    def block(h, first):
        for c in (first, first + 1):
            rows = parts[c]
            q, k, v, g = (ref[h, rows] for ref in (q_ref, k_ref, v_ref, g_ref))
            w_0 = wb[0, rows]
            q_f = q.astype(F32)
            q_0 = (w_0 * q_f).astype(BF16)
            g_0 = (w_0 * g.astype(F32)).astype(BF16)
            raw_t = jnp.where(upper, mm(k, q, 1, 1), 0.0).astype(BF16)
            pv[h, rows] = mm(raw_t, g_0, 1, 0)
            da_t = jnp.where(upper, mm(v, g, 1, 1), 0.0).astype(BF16)
            pk[h, rows] = mm(da_t, q_0, 1, 0)
            z_0 = mm(da_t, k, 0, 0)
            if c:
                both = mm(g, jnp.concatenate([prefix[h, c - 1], st0[h]], axis=0), 1, 1)
                z_0, z_1 = z_0 + both[:, :dim], both[:, dim:]
            else:
                z_1 = mm(g, st0[h], 1, 1)
            tot[h, rows] = w_0 * z_0 + wb[1, rows] * z_1
            if h == 0:
                acc[0, rows] = q_f * z_0
                acc[1, rows] = q_f * z_1
            else:
                acc[0, rows] += q_f * z_0
                acc[1, rows] += q_f * z_1

    def level_pair(h, stage, fresh):
        both_states = jnp.concatenate([st[stage, h], st[stage + 1, h]], axis=0).astype(BF16)
        row = 2 + stage
        for rows in parts:
            both = mm(g_ref[h, rows], both_states, 1, 1)
            q_f = q_ref[h, rows].astype(F32)
            total = tot[h, rows]
            for i in range(2):
                z_i = both[:, i * dim : (i + 1) * dim]
                total = total + wb[row + i, rows] * z_i
                if fresh:
                    acc[row + i, rows] = q_f * z_i
                else:
                    acc[row + i, rows] += q_f * z_i
            if stage == 0:
                tot[h, rows] = total
            else:
                qg_ref[h, rows] = total.astype(BF16)

    def apply(h, grad_0):
        grad = gg[h] + flag(core == 0) * grad_0
        zero = jnp.zeros((dim, dim), BF16)
        for c, rows in enumerate(parts):
            x = (grad + suffix[h, c] if c < chunks - 1 else grad).astype(BF16)
            wide = jnp.concatenate([jnp.concatenate([x.T, zero], axis=1), jnp.concatenate([zero, x], axis=1)], axis=0)
            both = mm(jnp.concatenate([v_ref[h, rows], k_ref[h, rows]], axis=1), wide, 1, 0)
            kg_ref[h, rows] = (pk[h, rows] + both[:, :dim]).astype(BF16)
            vg_ref[h, rows] = (pv[h, rows] + both[:, dim:]).astype(BF16)

    def take_up(s, p):
        f_copy(s, p).wait_recv()
        got = f_got[s, p]
        if s < 3:
            f_run[s + 1, p] = f_run[s, p] + got
            f_copy(s + 1, p).start()
        st[s, own + p] = bits[s] * got
        state_copy(s, p).start()
        b_copy(s, p).wait_recv()
        total = b_got[s, p] if s == 0 else adj[p] + b_got[s, p]
        if s < 3:
            adj[p] = total
            b_msg[s + 1, p] = total + bits[2 - s] * level_sum(p, 3 - s)
            b_copy(s + 1, p).start()
        else:
            gg[own + p] = total
            grad_copy(p).start()

    def middle(p):
        for stage in (0, 1):
            state_copy(stage, p).wait_recv()
        level_pair(own + p, 0, p == 0)
        level_pair(other + p, 0, False)

    work = [(h, c) for h in range(heads) for c in range(0, chunks, 2)]
    block(*work.pop(0))
    for index, (s, p) in enumerate(ARRIVALS):
        take_up(s, p)
        for _ in range(BLOCKS[index]):
            block(*work.pop(0))
        for piece in MIDDLES[index]:
            middle(piece)
    for p in range(half):
        level_pair(own + p, 2, p == 0)
    for p in range(half):
        for stage in (2, 3):
            state_copy(stage, p).wait_recv()
        level_pair(other + p, 2, False)
    ones = jnp.ones((8, dim), BF16)
    for row in range(levels + 1):
        term = acc[row]
        high = term.astype(BF16)
        low = (term - high.astype(F32)).astype(BF16)
        sums = mm(ones, high, 1, 1) + mm(ones, low, 1, 1)
        slots[mine, row : row + 1, :] = sums[0:1]
    for i in range(head_count - 1):
        row_copy(i).start()
    for p in range(half):
        apply(own + p, in_own[p, 3])
    for p in range(half):
        grad_copy(p).wait_recv()
        apply(other + p, in_other[p, 1])
    for i in range(head_count - 1):
        row_copy(i).wait_recv()
    total = slots[0]
    for index in range(1, head_count):
        total = total + slots[index]
    wg_ref[...] = total

    for i in range(half):
        early_copy(i).wait_send()
        late_copy(i).wait_send()
        low_copy(i).wait_send()
        grad_copy(i).wait_send()
    for s, p in ARRIVALS:
        f_copy(s, p).wait_send()
        b_copy(s, p).wait_send()
        state_copy(s, p).wait_send()
    for i in range(head_count - 1):
        row_copy(i).wait_send()


def copy_out_kernel(*refs):
    count = len(refs) // 2
    sems = refs[-1]
    copies = [pltpu.make_async_copy(refs[i], refs[count + i], sems.at[i]) for i in range(count)]
    for copy in copies:
        copy.start()
    for copy in copies:
        copy.wait()


def copy_out(arrays):
    return pl.pallas_call(
        copy_out_kernel,
        in_specs=[pl.BlockSpec(memory_space=pltpu.VMEM)] * len(arrays),
        out_specs=[pl.BlockSpec(memory_space=pl.ANY)] * len(arrays),
        out_shape=[jax.ShapeDtypeStruct(array.shape, array.dtype) for array in arrays],
        scratch_shapes=[pltpu.SemaphoreType.DMA((len(arrays),))],
        compiler_params=pltpu.CompilerParams(vmem_limit_bytes=1 << 20),
    )(*arrays)


def per_device(queries, key_rows, value_rows, level_weight, out_grad):
    heads, length, dim = queries.shape
    half, rows = heads // 2, level_weight.shape[0]
    vmem, hbm = pl.BlockSpec(memory_space=pltpu.VMEM), pl.BlockSpec(memory_space=pltpu.HBM)

    def f32(*shape):
        return pltpu.VMEM(shape, F32)

    def square(*lead):
        return f32(*lead, dim, dim)

    def pairs(*shape):
        return pltpu.SemaphoreType.DMA((2, *shape))

    tokens = pltpu.VMEM((heads, length, dim), BF16)
    arrays = pl.pallas_call(
        whole_kernel,
        in_specs=[hbm] * 4 + [vmem],
        out_specs=[vmem] * 4,
        out_shape=[jax.ShapeDtypeStruct(queries.shape, BF16)] * 3 + [jax.ShapeDtypeStruct(level_weight.shape, F32)],
        scratch_shapes=[tokens] * 4
        + [f32(heads, length, dim)] * 3
        + [f32(rows, length, dim)] * 2
        + [square(heads, 6), square(half, 6), square(half, 2)]
        + [square(4, half)] * 4
        + [square(half), pltpu.VMEM((heads, dim, dim), BF16), square(4, heads), square(heads)]
        + [pltpu.VMEM((heads, length // CHUNK - 1, dim, dim), BF16), square(heads, length // CHUNK - 1)]
        + [f32(4, rows, length)]
        + [pltpu.SemaphoreType.DMA((heads, 4))]
        + [pairs(3 * half), pairs(4, half), pairs(4, half), pairs(4, half), pairs(half), pairs(3)],
        compiler_params=pltpu.CompilerParams(
            collective_id=0, has_side_effects=True, vmem_limit_bytes=47 << 20),
    )(queries, key_rows, value_rows, out_grad, level_weight)
    return tuple(copy_out(arrays))


def solution(mesh):
    rows = P("head", "ctx", None)
    return jax.shard_map(
        per_device,
        mesh=mesh,
        in_specs=(rows, rows, rows, P(None, "ctx"), rows),
        out_specs=(rows, rows, rows, P(None, "ctx")),
        check_vma=False,
    )
```
